16 devices in a mesh: rep: 4 (over y, z, core), dp: 4 (over x).
Axes of the slice: x: 4, y: 2, z: 1, core: 2. Of those that a mesh axis runs over, the one named last changes fastest.
The devices are a block of a 4x4x8 slice.
Arguments:
- x: bfloat16 [16, 4096, 512], P(('rep', 'dp')), parts along dimension 0
- dy: bfloat16 [16, 4096, 512], P(('rep', 'dp')), parts along dimension 0
- w_gate: bfloat16 [2, 512, 2048], replicated
- w_up: bfloat16 [2, 512, 2048], replicated
- w_down: bfloat16 [2, 2048, 512], replicated
- m_w_gate: float32 [2, 512, 2048], replicated
- m_w_up: float32 [2, 512, 2048], replicated
- m_w_down: float32 [2, 2048, 512], replicated
- v_w_gate: float32 [2, 512, 2048], replicated
- v_w_up: float32 [2, 512, 2048], replicated
- v_w_down: float32 [2, 2048, 512], replicated
Outputs:
- output 1: bfloat16 [8, 512, 2048], P('rep'), parts along dimension 0
- output 2: bfloat16 [8, 512, 2048], P('rep'), parts along dimension 0
- output 3: bfloat16 [8, 2048, 512], P('rep'), parts along dimension 0
- output 4: float32 [8, 512, 2048], P('rep'), parts along dimension 0
- output 5: float32 [8, 512, 2048], P('rep'), parts along dimension 0
- output 6: float32 [8, 2048, 512], P('rep'), parts along dimension 0
- output 7: float32 [8, 512, 2048], P('rep'), parts along dimension 0
- output 8: float32 [8, 512, 2048], P('rep'), parts along dimension 0
- output 9: float32 [8, 2048, 512], P('rep'), parts along dimension 0
There are 4 independent parts. The reference program is written for one: setup_inputs(seed, part) draws one part's arguments, and reference() takes and returns one part's arrays. A program takes and returns all parts, laid end to end along the dimension named above; an argument that names none is the same for every part.
All inputs are finite; a program needn't handle non-finite values.
Results may differ from the reference program's by a relative error of at most 0.02.
Values are sent between devices in bfloat16 or wider.
A program may use at most 768 MiB of HBM per device.

```python
import jax
import jax.numpy as jnp
from jax import lax

SEQUENCES = 4
TOKENS = 4096
D = 512
FF = 2048
LAYERS = 2
NAMES = ("w_gate", "w_up", "w_down")
SHAPES = {"w_gate": (LAYERS, D, FF), "w_up": (LAYERS, D, FF), "w_down": (LAYERS, FF, D)}


def bump(key, n, height):
    away = (jnp.arange(n, dtype=jnp.int32) - jax.random.randint(key, (), 0, n, jnp.int32)) % n
    return jnp.where(away < n // 8, height, 1.0)


def together(key, own, strength):
    shared = jax.random.normal(key, own.shape[1:], jnp.float32)
    return (own + strength * shared) * lax.rsqrt(1 + strength * strength)


def setup_inputs(seed: int = 0, part: int = 0) -> dict:
    kx, kdy, ka, kb, kz, kf, kh, kl, *keys = jax.random.split(jax.random.key(seed), 8 + 3 * len(NAMES))
    kx, kdy, ka, kb = (jax.random.fold_in(k, part) for k in (kx, kdy, ka, kb))
    kw, km, kv = (keys[i::3] for i in range(3))
    shape = (SEQUENCES, TOKENS, D)
    much_x, much_dy = jax.random.uniform(kz, (2,), jnp.float32, 0.0, 1.0)
    loud = 2.0 ** jax.random.uniform(jax.random.fold_in(kz, 1), (), jnp.float32, -1.0, 2.0)
    layers = 2.0 ** jax.random.uniform(kl, (LAYERS, 1, 1), jnp.float32, -1.0, 1.0)
    x = together(ka, jax.random.normal(kx, shape, jnp.float32), much_x) * bump(kf, D, 4.0)
    dy = together(kb, jax.random.normal(kdy, shape, jnp.float32), much_dy)
    drawn = {"x": x.astype(jnp.bfloat16), "dy": (loud * dy * (SEQUENCES * TOKENS) ** -0.5).astype(jnp.bfloat16)}
    for key, name in zip(kw, NAMES, strict=True):
        w = jax.random.normal(key, SHAPES[name], jnp.float32) * SHAPES[name][1] ** -0.5
        drawn[name] = (w * {"w_gate": 1.0, "w_up": bump(kh, FF, 4.0), "w_down": layers}[name]).astype(jnp.bfloat16)
    for key, name in zip(km, NAMES, strict=True):
        drawn[f"m_{name}"] = 0.1 * jax.random.normal(key, SHAPES[name], jnp.float32)
    for key, name in zip(kv, NAMES, strict=True):
        drawn[f"v_{name}"] = jax.random.uniform(key, SHAPES[name], jnp.float32, 0.005, 0.015)
    return drawn


def matmul(a, w):
    return jnp.dot(a, w, preferred_element_type=jnp.float32).astype(jnp.bfloat16)


def normed(h):
    wide = h.astype(jnp.float32)
    scale = lax.rsqrt(jnp.mean(wide**2, -1, keepdims=True) + 1e-6)
    return (wide * scale).astype(jnp.bfloat16)


def layer(h, w):
    a = normed(h)
    gate = jnp.dot(a, w["w_gate"], preferred_element_type=jnp.float32)
    up = jnp.dot(a, w["w_up"], preferred_element_type=jnp.float32)
    return h + matmul((jax.nn.silu(gate) * up).astype(jnp.bfloat16), w["w_down"])


def adamw(w, m, v, g):
    m = 0.9 * m + 0.1 * g
    v = 0.95 * v + 0.05 * g * g
    step = m * lax.rsqrt(v + 1e-8) + 0.1 * w
    return (w - 0.02 * step).astype(jnp.bfloat16), m, v


def stack(weights, h):
    return lax.scan(lambda h, w: (layer(h, w), None), h, weights)[0]


def reference(x, dy, w_gate, w_up, w_down, m_w_gate, m_w_up, m_w_down, v_w_gate, v_w_up, v_w_down):
    weights = dict(zip(NAMES, (w_gate, w_up, w_down), strict=True))

    def take(so_far, sequence):
        h, by_y = sequence
        _, back = jax.vjp(lambda w: stack(w, h), weights)
        return jax.tree.map(lambda total, term: total + term.astype(jnp.float32), so_far, back(by_y)[0]), None

    none_yet = {name: jnp.zeros(w.shape, jnp.float32) for name, w in weights.items()}
    by_weights, _ = lax.scan(take, none_yet, (x, dy))
    gradients = [by_weights[name].astype(jnp.bfloat16).astype(jnp.float32) for name in NAMES]
    new = [
        adamw(w.astype(jnp.float32), m, v, g)
        for w, m, v, g in zip((w_gate, w_up, w_down), (m_w_gate, m_w_up, m_w_down), (v_w_gate, v_w_up, v_w_down), gradients, strict=True)
    ]
    return tuple(one[which] for which in range(3) for one in new)
```

```python
import functools

import jax
import jax.numpy as jnp
from jax import lax
from jax.experimental import pallas as pl
from jax.experimental.pallas import tpu as pltpu
from jax.sharding import PartitionSpec as P

F32 = jnp.float32
BF16 = jnp.bfloat16
CHUNK = 256
TILE = 512
GSLOTS = 4


def dot(a, b):
    return jnp.dot(a, b, preferred_element_type=F32)


def dot_t(a, b):
    return lax.dot_general(a, b, (((1,), (1,)), ((), ())), preferred_element_type=F32)


def sigmoid(z):
    return 0.5 * jnp.tanh(0.5 * z) + 0.5


def norm_scale(wide):
    return lax.rsqrt(jnp.mean(wide * wide, -1, keepdims=True) + 1e-6)


def step_kernel(
    n, comm,
    x_hbm, dy_hbm, wg_hbm, wu_hbm, wd_hbm, g_hbm,
    a_all, a_t, d_all, d_t, da, h_all, hid_all, dgu_all, w0_gu, w0_d, s_gu, s_d, part, r1, r2, grad,
    in_sem, w_sem, out_sem, send_sem, recv_sem,
):
    tokens, width = h_all.shape
    layers, _, ff = wg_hbm.shape
    chunks = ff // CHUNK
    tiles = tokens // TILE
    total = layers * chunks
    rows = width // n
    half = rows // 2
    top = layers - 1
    me = lax.axis_index("dp")
    right, left = lax.rem(me + 1, n), lax.rem(me + n - 1, n)
    across = lax.rem(me + 2, n)

    def load(src, dst, sem):
        return pltpu.make_async_copy(src, dst, sem)

    first = [
        load(wg_hbm.at[0], w0_gu.at[0], in_sem.at[0]),
        load(wu_hbm.at[0], w0_gu.at[1], in_sem.at[1]),
        load(wd_hbm.at[0], w0_d, in_sem.at[2]),
    ]

    def x_load(t):
        r = pl.ds(pl.multiple_of(t * TILE, TILE), TILE)
        return load(x_hbm.at[0, r], a_all.at[0, r], in_sem.at[4 + 2 * t])

    def dy_load(t):
        r = pl.ds(pl.multiple_of(t * TILE, TILE), TILE)
        return load(dy_hbm.at[0, r], d_all.at[r], in_sem.at[5 + 2 * t])

    def w_loads(s):
        layer = top - s // chunks
        c = pl.ds(pl.multiple_of(lax.rem(s, chunks) * CHUNK, CHUNK), CHUNK)
        slot = lax.rem(s, 2)
        return [
            load(wg_hbm.at[layer, :, c], s_gu.at[slot, :, pl.ds(0, CHUNK)], w_sem.at[slot, 0]),
            load(wu_hbm.at[layer, :, c], s_gu.at[slot, :, pl.ds(CHUNK, CHUNK)], w_sem.at[slot, 1]),
            load(wd_hbm.at[layer, c], s_d.at[slot], w_sem.at[slot, 2]),
        ]

    x_load(0).start()
    for copy in first:
        copy.start()
    for t in range(1, tiles):
        x_load(t).start()
    for t in range(tiles):
        dy_load(t).start()
    for copy in w_loads(0):
        copy.start()
    if comm:
        barrier = pltpu.get_barrier_semaphore()
        for other in (left, right):
            pl.semaphore_signal(barrier, inc=1, device_id={"dp": other}, device_id_type=pl.DeviceIdType.MESH)
    x_load(0).wait()
    for copy in first:
        copy.wait()

    def forward(t, carry):
        @pl.when(t > 0)
        def _():
            x_load(t).wait()

        dy_load(t).wait()
        r = pl.ds(pl.multiple_of(t * TILE, TILE), TILE)
        x = a_all[0, r].astype(F32)
        a = (x * norm_scale(x)).astype(BF16)
        a_all[0, r] = a
        acc = None
        step = 512
        for c in range(ff // step):
            cols = pl.ds(c * step, step)
            gate = dot(a, w0_gu[0, :, cols])
            up = dot(a, w0_gu[1, :, cols])
            hid = (gate * sigmoid(gate) * up).astype(BF16)
            term = dot(hid, w0_d[cols])
            acc = term if acc is None else acc + term
        h = (x + acc.astype(BF16).astype(F32)).astype(BF16)
        h_all[r] = h
        wide = h.astype(F32)
        a = (wide * norm_scale(wide)).astype(BF16)
        a_all[1, r] = a
        a_t[:, r] = a.T
        d_t[:, r] = d_all[r].T
        return carry

    lax.fori_loop(0, tiles, forward, 0)

    def piece(j, which):
        if which is None:
            return pl.ds(pl.multiple_of(j * rows, rows), rows)
        return pl.ds(pl.multiple_of(j * rows + which * half, half), half)

    def copies(kind, q):
        par = lax.rem(q, 2)
        g = lax.rem(q, GSLOTS)
        if kind == 0:
            pairs = [(part.at[par, :, piece(across, d)], r1.at[par, d]) for d in range(2)]
        elif kind == 1:
            pairs = [(part.at[par, :, piece(to, None)], r2.at[par, d]) for d, to in enumerate((right, left))]
        elif kind == 2:
            own = grad.at[g, :, piece(me, None)]
            pairs = [(own, own), (own, own)]
        else:
            pairs = [(grad.at[g, :, piece(who, d)],) * 2 for d, who in enumerate((left, right))]
        return [
            pltpu.make_async_remote_copy(
                src_ref=src, dst_ref=dst, send_sem=send_sem.at[kind, d, par], recv_sem=recv_sem.at[kind, d, par],
                device_id={"dp": to}, device_id_type=pl.DeviceIdType.MESH,
            )
            for d, ((src, dst), to) in enumerate(zip(pairs, (right, left)))
        ]

    def landed(kind, q):
        par = lax.rem(q, 2)
        g = lax.rem(q, GSLOTS)
        if kind == 0:
            refs = [r1.at[par, d] for d in range(2)]
        elif kind == 1:
            refs = [r2.at[par, d] for d in range(2)]
        elif kind == 2:
            refs = [grad.at[g, :, piece(who, None)] for who in (left, right)]
        else:
            refs = [grad.at[g, :, piece(across, d)] for d in range(2)]
        for d, (ref, copy) in enumerate(zip(refs, copies(kind, q))):
            pltpu.make_async_remote_copy(
                src_ref=ref, dst_ref=ref, send_sem=send_sem.at[kind, d, par], recv_sem=recv_sem.at[kind, d, par],
                device_id={"dp": (left, right)[d]}, device_id_type=pl.DeviceIdType.MESH,
            ).wait_recv()
            copy.wait_send()

    def send(kind, q):
        for copy in copies(kind, q):
            copy.start()

    def pass_on(q):
        landed(0, q)
        par = lax.rem(q, 2)
        for d, to in enumerate((right, left)):
            at = piece(to, d)
            part[par, :, at] = (part[par, :, at].astype(F32) + r1[par, d].astype(F32)).astype(BF16)
        send(1, q)

    def finish(q):
        landed(1, q)
        par = lax.rem(q, 2)
        mine = part[par, :, piece(me, None)].astype(F32)
        grad[lax.rem(q, GSLOTS), :, piece(me, None)] = (mine + r2[par, 0].astype(F32) + r2[par, 1].astype(F32)).astype(BF16)
        send(2, q)

    def forward_on(q):
        landed(2, q)
        send(3, q)

    def out_copy(q):
        return pltpu.make_async_copy(grad.at[lax.rem(q, GSLOTS)], g_hbm.at[q], out_sem.at[lax.rem(q, 2)])

    def complete(q):
        landed(3, q)
        out_copy(q).start()

    def tile_body(layer, slot, t, with_da, fresh):
        r = pl.ds(pl.multiple_of(t * TILE, TILE), TILE)
        gu = dot(a_all[layer, r], s_gu[slot])
        gate, up = gu[:, :CHUNK], gu[:, CHUNK:]
        dhid = dot_t(d_all[r], s_d[slot]).astype(BF16).astype(F32)
        sig = sigmoid(gate)
        silu = gate * sig
        hid_all[r] = (silu * up).astype(BF16)
        dgate = (dhid * up * (sig + silu * (1.0 - sig))).astype(BF16)
        dup = (dhid * silu).astype(BF16)
        dgu_all[r, :CHUNK] = dgate
        dgu_all[r, CHUNK:] = dup
        if with_da:
            term = dot_t(jnp.concatenate([dgate, dup], axis=1), s_gu[slot])
            da[r] = jnp.where(fresh, 0.0, da[r]) + term

    def service(guard, fn, q):
        if not comm:
            return
        if guard is None:
            fn(q)
        else:
            pl.when(guard)(lambda: fn(q))

    def chunk_step(s, with_da):
        layer = top - s // chunks
        slot = lax.rem(s, 2)
        for copy in w_loads(s):
            copy.wait()

        @pl.when(s + 1 < total)
        def _():
            for copy in w_loads(s + 1):
                copy.start()

        service(s >= 3, forward_on, s - 3)
        fresh = lax.rem(s, chunks) == 0
        body = lambda t, c: (tile_body(layer, slot, t, with_da, fresh), c)[1]
        lax.fori_loop(0, tiles // 2, body, 0)
        service(s >= 2, finish, s - 2)
        lax.fori_loop(tiles // 2, tiles, body, 0)
        service(s >= 1, pass_on, s - 1)
        service(s >= 4, lambda q: out_copy(q).wait(), s - 4)
        dw = dot(a_t[...], dgu_all[...])
        part[slot, 0] = dw[:, :CHUNK].astype(BF16)
        part[slot, 1] = dw[:, CHUNK:].astype(BF16)
        dd = dot(d_t[...], hid_all[...])
        for k in range(width // CHUNK):
            b = pl.ds(k * CHUNK, CHUNK)
            part[slot, 2, b] = dd[k * CHUNK : (k + 1) * CHUNK].T.astype(BF16)
        if comm:
            send(0, s)
        else:
            pltpu.make_async_copy(part.at[slot], g_hbm.at[s], out_sem.at[slot]).start()
            pltpu.make_async_copy(part.at[slot], g_hbm.at[s], out_sem.at[slot]).wait()
        service(s >= 3, complete, s - 3)

    def turn(t, carry):
        r = pl.ds(pl.multiple_of(t * TILE, TILE), TILE)
        by_a = da[r].astype(BF16).astype(F32)
        h = h_all[r].astype(F32)
        scale = norm_scale(h)
        inner = jnp.mean(by_a * h, -1, keepdims=True)
        by_h = d_all[r].astype(F32) + (by_a * scale - h * (scale * scale * scale * inner))
        by_h = by_h.astype(BF16)
        d_all[r] = by_h
        d_t[:, r] = by_h.T
        a_t[:, r] = a_all[0, r].T
        return carry

    if comm:
        pl.semaphore_wait(barrier, 2)

    def upper(s, carry):
        chunk_step(s, True)
        return carry

    def lower(s, carry):
        chunk_step(s, False)
        return carry

    lax.fori_loop(0, chunks, upper, 0)
    lax.fori_loop(0, tiles, turn, 0)
    lax.fori_loop(chunks, total, lower, 0)

    def drain(s, carry):
        service(s <= total + 2, forward_on, s - 3)
        service(s <= total + 1, finish, s - 2)
        service(s <= total, pass_on, s - 1)
        service(None, lambda q: out_copy(q).wait(), s - 4)
        service(s <= total + 2, complete, s - 3)
        return carry

    if comm:
        lax.fori_loop(total, total + 4, drain, 0)


def gradients(n, x, dy, wg, wu, wd, comm=True):
    _, tokens, width = x.shape
    layers, _, ff = wg.shape
    assert layers == 2 and n == 4
    total = layers * ff // CHUNK
    rows = width // n
    anywhere = pl.BlockSpec(memory_space=pl.ANY)
    tiles = tokens // TILE
    return pl.pallas_call(
        functools.partial(step_kernel, n, comm),
        out_shape=jax.ShapeDtypeStruct((total, 3, width, CHUNK), BF16),
        in_specs=[anywhere] * 5,
        out_specs=anywhere,
        scratch_shapes=[
            pltpu.VMEM((2, tokens, width), BF16),
            pltpu.VMEM((width, tokens), BF16),
            pltpu.VMEM((tokens, width), BF16),
            pltpu.VMEM((width, tokens), BF16),
            pltpu.VMEM((tokens, width), F32),
            pltpu.VMEM((tokens, width), BF16),
            pltpu.VMEM((tokens, CHUNK), BF16),
            pltpu.VMEM((tokens, 2 * CHUNK), BF16),
            pltpu.VMEM((2, width, ff), BF16),
            pltpu.VMEM((ff, width), BF16),
            pltpu.VMEM((2, width, 2 * CHUNK), BF16),
            pltpu.VMEM((2, CHUNK, width), BF16),
            pltpu.VMEM((2, 3, width, CHUNK), BF16),
            pltpu.VMEM((2, 2, 3, rows // 2, CHUNK), BF16),
            pltpu.VMEM((2, 2, 3, rows, CHUNK), BF16),
            pltpu.VMEM((GSLOTS, 3, width, CHUNK), BF16),
            pltpu.SemaphoreType.DMA((4 + 2 * tiles,)),
            pltpu.SemaphoreType.DMA((2, 3)),
            pltpu.SemaphoreType.DMA((2,)),
            pltpu.SemaphoreType.DMA((4, 2, 2)),
            pltpu.SemaphoreType.DMA((4, 2, 2)),
        ],
        compiler_params=pltpu.CompilerParams(
            collective_id=0 if comm else None, has_side_effects=True, vmem_limit_bytes=67043328
        ),
        name="gradients",
    )(x, dy, wg, wu, wd)


def adamw_kernel(g_ref, *refs):
    ins, outs = refs[:9], refs[9:]
    for i in range(3):
        w, m, v = (ins[k * 3 + i][0] for k in range(3))
        if i < 2:
            g = g_ref[0, i].astype(F32)
        else:
            g = jnp.concatenate([g_ref[0, i, k * CHUNK : (k + 1) * CHUNK] for k in range(g_ref.shape[2] // CHUNK)], axis=1).astype(F32)
        m = 0.9 * m + 0.1 * g
        v = 0.95 * v + 0.05 * g * g
        step = m * lax.rsqrt(v + 1e-8) + 0.1 * w.astype(F32)
        outs[i][0] = (w.astype(F32) - 0.02 * step).astype(BF16)
        outs[3 + i][0] = m
        outs[6 + i][0] = v


def adamw(g, arrays):
    layers, width, ff = arrays[0].shape
    chunks = ff // CHUNK
    wide = pl.BlockSpec((1, width, CHUNK), lambda s: (layers - 1 - s // chunks, 0, lax.rem(s, chunks)))
    tall = pl.BlockSpec((1, CHUNK, width), lambda s: (layers - 1 - s // chunks, lax.rem(s, chunks), 0))
    specs = [wide, wide, tall] * 3
    return pl.pallas_call(
        adamw_kernel,
        grid=(layers * chunks,),
        out_shape=[jax.ShapeDtypeStruct(a.shape, a.dtype) for a in arrays],
        in_specs=[pl.BlockSpec((1, 3, width, CHUNK), lambda s: (s, 0, 0, 0))] + specs,
        out_specs=specs,
        compiler_params=pltpu.CompilerParams(vmem_limit_bytes=48 * 1024 * 1024),
        name="adamw",
    )(g, *arrays)


def solution(mesh):
    n = mesh.shape["dp"]

    def step(x, dy, *arrays):
        g = gradients(n, x, dy, *arrays[:3])
        return tuple(adamw(g, arrays))

    return jax.shard_map(
        step,
        mesh=mesh,
        in_specs=(P(("rep", "dp"), None, None),) * 2 + (P(None, None, None),) * 9,
        out_specs=(P("rep", None, None),) * 9,
        check_vma=False,
    )
```

```python
import functools

import jax
import jax.numpy as jnp
from jax import lax
from jax.experimental import pallas as pl
from jax.experimental.pallas import tpu as pltpu
from jax.sharding import PartitionSpec as P

F32 = jnp.float32
BF16 = jnp.bfloat16
CHUNK = 256
TILE = 1024
GSLOTS = 4
FORWARD_PIECES = 4
FORWARD_TILE = 512


def dot(a, b):
    return jnp.dot(a, b, preferred_element_type=F32)


def dot_t(a, b):
    return lax.dot_general(a, b, (((1,), (1,)), ((), ())), preferred_element_type=F32)


def sigmoid(z):
    return 0.5 * jnp.tanh(0.5 * z) + 0.5


def norm_scale(wide):
    return lax.rsqrt(jnp.mean(wide * wide, -1, keepdims=True) + 1e-6)


def step_kernel(
    n, comm,
    x_hbm, dy_hbm, wg_hbm, wu_hbm, wd_hbm, near_hbm, to_right_hbm, to_left_hbm,
    a_all, a_t, d_all, d_t, da, h_all, hid_all, dgu_all, w0_gu, w0_d, s_gu, s_d, part, r1, r2, grad,
    in_sem, w0_sem, w_sem, out_sem, send_sem, recv_sem,
):
    tokens, width = h_all.shape
    layers, _, ff = wg_hbm.shape
    chunks = ff // CHUNK
    tiles = tokens // TILE
    total = layers * chunks
    rows = width // n
    half = rows // 2
    top = layers - 1
    me = lax.axis_index("dp")
    right, left = lax.rem(me + 1, n), lax.rem(me + n - 1, n)
    across = lax.rem(me + 2, n)

    def load(src, dst, sem):
        return pltpu.make_async_copy(src, dst, sem)

    piece_ff = ff // FORWARD_PIECES

    def w0_loads(c):
        cols = pl.ds(c * piece_ff, piece_ff)
        return [
            load(wg_hbm.at[0, :, cols], w0_gu.at[0, :, cols], w0_sem.at[c, 0]),
            load(wu_hbm.at[0, :, cols], w0_gu.at[1, :, cols], w0_sem.at[c, 1]),
            load(wd_hbm.at[0, cols], w0_d.at[cols], w0_sem.at[c, 2]),
        ]

    def x_load(t):
        r = pl.ds(pl.multiple_of(t * FORWARD_TILE, FORWARD_TILE), FORWARD_TILE)
        return load(x_hbm.at[0, r], h_all.at[r], in_sem.at[t, 0])

    def dy_load(t):
        r = pl.ds(pl.multiple_of(t * FORWARD_TILE, FORWARD_TILE), FORWARD_TILE)
        return load(dy_hbm.at[0, r], d_all.at[r], in_sem.at[t, 1])

    def w_loads(s):
        layer = top - s // chunks
        c = pl.ds(pl.multiple_of(lax.rem(s, chunks) * CHUNK, CHUNK), CHUNK)
        slot = lax.rem(s, 2)
        return [
            load(wg_hbm.at[layer, :, c], s_gu.at[slot, :, pl.ds(0, CHUNK)], w_sem.at[slot, 0]),
            load(wu_hbm.at[layer, :, c], s_gu.at[slot, :, pl.ds(CHUNK, CHUNK)], w_sem.at[slot, 1]),
            load(wd_hbm.at[layer, c], s_d.at[slot], w_sem.at[slot, 2]),
        ]

    x_load(0).start()
    for c in range(FORWARD_PIECES):
        for copy in w0_loads(c):
            copy.start()
    barrier = pltpu.get_barrier_semaphore() if comm else None
    if comm:
        for other in (left, right):
            pl.semaphore_signal(barrier, inc=1, device_id={"dp": other}, device_id_type=pl.DeviceIdType.MESH)
    x_load(0).wait()

    def token_rows(t):
        return pl.ds(pl.multiple_of(t * FORWARD_TILE, FORWARD_TILE), FORWARD_TILE)

    def before(t):
        r = token_rows(t)
        x = h_all[r].astype(F32)
        a_all[0, r] = (x * norm_scale(x)).astype(BF16)

    def after(t):
        r = token_rows(t)
        h = (h_all[r].astype(F32) + da[r].astype(BF16).astype(F32)).astype(BF16)
        h_all[r] = h
        wide = h.astype(F32)
        a = (wide * norm_scale(wide)).astype(BF16)
        a_all[1, r] = a
        a_t[:, r] = a.T
        d_t[:, r] = d_all[r].T

    def forward(t, opening):
        a = a_all[0, token_rows(t)]
        acc = None
        for c in range(FORWARD_PIECES):
            cols = pl.ds(c * piece_ff, piece_ff)
            if opening:
                for copy in w0_loads(c):
                    copy.wait()
                if c == 0:
                    for other in range(tokens // FORWARD_TILE):
                        if other:
                            x_load(other).start()
                        dy_load(other).start()
                    for copy in w_loads(0):
                        copy.start()
            gate = dot(a, w0_gu[0, :, cols])
            up = dot(a, w0_gu[1, :, cols])
            if c == 0 and not opening:
                after(t - 1)
            if c == 1 and not opening:
                before(jnp.minimum(t + 1, tokens // FORWARD_TILE - 1))
            hid = (gate * sigmoid(gate) * up).astype(BF16)
            term = dot(hid, w0_d[cols])
            acc = term if acc is None else acc + term
        da[token_rows(t)] = acc

    before(0)
    forward(0, True)
    for t in range(tokens // FORWARD_TILE):
        if t:
            x_load(t).wait()
        dy_load(t).wait()
    before(1)

    def forward_rest(t, carry):
        forward(t, False)
        return carry

    lax.fori_loop(1, tokens // FORWARD_TILE, forward_rest, 0)
    after(tokens // FORWARD_TILE - 1)

    def piece(j, which):
        if which is None:
            return pl.ds(pl.multiple_of(j * rows, rows), rows)
        return pl.ds(pl.multiple_of(j * rows + which * half, half), half)

    def copies(kind, q):
        par = lax.rem(q, 2)
        g = lax.rem(q, GSLOTS)
        if kind == 0:
            pairs = [(part.at[par, :, piece(across, d)], r1.at[par, d]) for d in range(2)]
        elif kind == 1:
            pairs = [(part.at[par, :, piece(to, None)], r2.at[par, d]) for d, to in enumerate((right, left))]
        else:
            pairs = [(grad.at[g, 0], grad.at[g, 1 + d]) for d in range(2)]
        return [
            pltpu.make_async_remote_copy(
                src_ref=src, dst_ref=dst, send_sem=send_sem.at[kind, d, par], recv_sem=recv_sem.at[kind, d, par],
                device_id={"dp": to}, device_id_type=pl.DeviceIdType.MESH,
            )
            for d, ((src, dst), to) in enumerate(zip(pairs, (right, left)))
        ]

    def landed(kind, q):
        for copy in copies(kind, q):
            copy.wait_recv()
            copy.wait_send()

    def send(kind, q):
        for copy in copies(kind, q):
            copy.start()

    def pass_on(q):
        landed(0, q)
        par = lax.rem(q, 2)
        for d, to in enumerate((right, left)):
            at = piece(to, d)
            part[par, :, at] = (part[par, :, at].astype(F32) + r1[par, d].astype(F32)).astype(BF16)
        send(1, q)

    def finish(q):
        landed(1, q)
        par = lax.rem(q, 2)
        mine = part[par, :, piece(me, None)].astype(F32)
        grad[lax.rem(q, GSLOTS), 0] = (mine + r2[par, 0].astype(F32) + r2[par, 1].astype(F32)).astype(BF16)
        send(2, q)

    def out_copies(q):
        g, par = lax.rem(q, GSLOTS), lax.rem(q, 2)
        return [
            pltpu.make_async_copy(grad.at[g], near_hbm.at[q], out_sem.at[par, 0]),
            pltpu.make_async_copy(grad.at[g, 1, :, pl.ds(0, half)], to_right_hbm.at[q], out_sem.at[par, 1]),
            pltpu.make_async_copy(grad.at[g, 2, :, pl.ds(half, half)], to_left_hbm.at[q], out_sem.at[par, 2]),
        ]

    def collect(q):
        landed(2, q)
        for copy in out_copies(q):
            copy.start()

    def settle(q):
        for copy in out_copies(q):
            copy.wait()

    def tile_body(layer, slot, t, with_da, fresh):
        r = pl.ds(pl.multiple_of(t * TILE, TILE), TILE)
        gu = dot(a_all[layer, r], s_gu[slot])
        gate, up = gu[:, :CHUNK], gu[:, CHUNK:]
        dhid = dot_t(d_all[r], s_d[slot]).astype(BF16).astype(F32)
        sig = sigmoid(gate)
        silu = gate * sig
        hid_all[r] = (silu * up).astype(BF16)
        dgate = (dhid * up * (sig + silu * (1.0 - sig))).astype(BF16)
        dup = (dhid * silu).astype(BF16)
        dgu_all[r, :CHUNK] = dgate
        dgu_all[r, CHUNK:] = dup
        if with_da:
            term = dot_t(jnp.concatenate([dgate, dup], axis=1), s_gu[slot])
            da[r] = jnp.where(fresh, 0.0, da[r]) + term

    def service(guard, fn, q):
        if not comm:
            return
        if guard is None:
            fn(q)
        else:
            pl.when(guard)(lambda: fn(q))

    def chunk_step(s, with_da):
        layer = top - s // chunks
        slot = lax.rem(s, 2)
        for copy in w_loads(s):
            copy.wait()

        @pl.when(s + 1 < total)
        def _():
            for copy in w_loads(s + 1):
                copy.start()

        fresh = lax.rem(s, chunks) == 0
        body = lambda t, c: (tile_body(layer, slot, t, with_da, fresh), c)[1]
        ahead = tiles - 1
        lax.fori_loop(0, ahead, body, 0)
        service(s >= 3, finish, s - 2)
        service(s >= 4, settle, s - 4)
        service(s >= 3, collect, s - 3)
        service(s >= 1, pass_on, s - 1)
        lax.fori_loop(ahead, tiles, body, 0)
        dw = dot(a_t[...], dgu_all[...])
        part[slot, 0] = dw[:, :CHUNK].astype(BF16)
        part[slot, 1] = dw[:, CHUNK:].astype(BF16)
        dd = dot(d_t[...], hid_all[...])
        for k in range(width // CHUNK):
            b = pl.ds(k * CHUNK, CHUNK)
            part[slot, 2, b] = dd[k * CHUNK : (k + 1) * CHUNK].T.astype(BF16)
        if comm:
            send(0, s)
        service(s == 1, finish, s - 1)

    def turn(t, carry):
        r = pl.ds(pl.multiple_of(t * TILE, TILE), TILE)
        by_a = da[r].astype(BF16).astype(F32)
        h = h_all[r].astype(F32)
        scale = norm_scale(h)
        inner = jnp.mean(by_a * h, -1, keepdims=True)
        by_h = d_all[r].astype(F32) + (by_a * scale - h * (scale * scale * scale * inner))
        by_h = by_h.astype(BF16)
        d_all[r] = by_h
        d_t[:, r] = by_h.T
        a_t[:, r] = a_all[0, r].T
        return carry

    if comm:
        pl.semaphore_wait(barrier, 2)

    def upper(s, carry):
        chunk_step(s, True)
        return carry

    def lower(s, carry):
        chunk_step(s, False)
        return carry

    lax.fori_loop(0, chunks, upper, 0)
    lax.fori_loop(0, tiles, turn, 0)
    lax.fori_loop(chunks, total, lower, 0)

    if comm:
        last = total - 1
        finish(last - 1)
        settle(last - 3)
        collect(last - 2)
        pass_on(last)
        finish(last)
        settle(last - 2)
        collect(last - 1)
        collect(last)
        settle(last - 1)
        settle(last)


def gradients(n, x, dy, wg, wu, wd, comm=True):
    _, tokens, width = x.shape
    layers, _, ff = wg.shape
    assert layers == 2 and n == 4
    total = layers * ff // CHUNK
    rows = width // n
    anywhere = pl.BlockSpec(memory_space=pl.ANY)
    return pl.pallas_call(
        functools.partial(step_kernel, n, comm),
        out_shape=[
            jax.ShapeDtypeStruct((total, 3, 3, rows, CHUNK), BF16),
            jax.ShapeDtypeStruct((total, 3, rows // 2, CHUNK), BF16),
            jax.ShapeDtypeStruct((total, 3, rows // 2, CHUNK), BF16),
        ],
        in_specs=[anywhere] * 5,
        out_specs=[anywhere] * 3,
        scratch_shapes=[
            pltpu.VMEM((2, tokens, width), BF16),
            pltpu.VMEM((width, tokens), BF16),
            pltpu.VMEM((tokens, width), BF16),
            pltpu.VMEM((width, tokens), BF16),
            pltpu.VMEM((tokens, width), F32),
            pltpu.VMEM((tokens, width), BF16),
            pltpu.VMEM((tokens, CHUNK), BF16),
            pltpu.VMEM((tokens, 2 * CHUNK), BF16),
            pltpu.VMEM((2, width, ff), BF16),
            pltpu.VMEM((ff, width), BF16),
            pltpu.VMEM((2, width, 2 * CHUNK), BF16),
            pltpu.VMEM((2, CHUNK, width), BF16),
            pltpu.VMEM((2, 3, width, CHUNK), BF16),
            pltpu.VMEM((2, 2, 3, rows // 2, CHUNK), BF16),
            pltpu.VMEM((2, 2, 3, rows, CHUNK), BF16),
            pltpu.VMEM((GSLOTS, 3, 3, rows, CHUNK), BF16),
            pltpu.SemaphoreType.DMA((tokens // FORWARD_TILE, 2)),
            pltpu.SemaphoreType.DMA((FORWARD_PIECES, 3)),
            pltpu.SemaphoreType.DMA((2, 3)),
            pltpu.SemaphoreType.DMA((2, 3)),
            pltpu.SemaphoreType.DMA((3, 2, 2)),
            pltpu.SemaphoreType.DMA((3, 2, 2)),
        ],
        compiler_params=pltpu.CompilerParams(
            collective_id=0 if comm else None, has_side_effects=True, vmem_limit_bytes=67043328
        ),
        name="gradients",
    )(x, dy, wg, wu, wd)


def adamw_math(w, m, v, g):
    m = 0.9 * m + 0.1 * g
    v = 0.95 * v + 0.05 * g * g
    step = m * lax.rsqrt(v + 1e-8) + 0.1 * w
    return (w - 0.02 * step).astype(BF16), m, v


def adamw_kernel(gs, me_ref, *refs):
    parts, ins, outs = refs[:gs], refs[gs : gs + 9], refs[-9:]
    group = parts[0].shape[0]
    for j in range(group):
        cols = pl.ds(j * CHUNK, CHUNK)
        for i in range(3):
            g = parts[0][j, 0, i] if gs == 1 else jnp.concatenate([p[j, i] for p in parts], axis=0)
            at = (0, slice(None), cols) if i < 2 else (0, j)
            new = adamw_math(ins[i][at].astype(F32), ins[3 + i][at], ins[6 + i][at], g.astype(F32))
            for k in range(3):
                outs[3 * k + i][at] = new[k]


def adamw(n, me, gs, arrays, group, near, before):
    layers, width, ff = arrays[0].shape
    groups = ff // CHUNK // group
    rows = width // n
    per = CHUNK // rows

    def row(rel, me):
        ahead = jnp.where(rel == 0, 0, jnp.where(rel == 1, n - 1, 1)) if near else n // 2
        return lax.rem(me[0] + ahead, n)

    def wide_map(s, rel, c, me):
        return layers - 1 - s, row(rel, me), c

    def tall_map(s, rel, c, me):
        at = row(rel, me)
        return layers - 1 - s, c, lax.rem(at, per), at // per

    wide = pl.BlockSpec((1, rows, group * CHUNK), wide_map, pipeline_mode=pl.Buffered(2))
    tall = pl.BlockSpec((1, group, rows, CHUNK), tall_map, pipeline_mode=pl.Buffered(2))
    specs = [wide, wide, tall] * 3
    outs = [pl.BlockSpec(b.block_shape, b.index_map) for b in specs]
    if near:
        g_specs = [pl.BlockSpec((group, 1, 3, rows, CHUNK), lambda s, rel, c, me: (s * groups + c, rel, 0, 0, 0))]
    else:
        g_specs = [pl.BlockSpec((group, 3, rows // 2, CHUNK), lambda s, rel, c, me: (s * groups + c, 0, 0, 0))] * 2
    shares = 3 if near else 1
    size = layers * ff * 3 * rows * shares
    return pl.pallas_call(
        functools.partial(adamw_kernel, len(gs)),
        grid_spec=pltpu.PrefetchScalarGridSpec(
            num_scalar_prefetch=1,
            grid=(layers, shares, groups),
            in_specs=g_specs + specs + [pl.BlockSpec(memory_space=pl.ANY)] * len(before),
            out_specs=outs,
        ),
        out_shape=[jax.ShapeDtypeStruct(a.shape, a.dtype) for a in arrays],
        input_output_aliases={1 + len(gs) + 9 + i: i for i in range(len(before))},
        compiler_params=pltpu.CompilerParams(vmem_limit_bytes=67043328),
        cost_estimate=pl.CostEstimate(flops=size * 2000, bytes_accessed=size * 22, transcendentals=size),
        name="adamw_near" if near else "adamw_across",
    )(me, *gs, *arrays, *before)


def solution(mesh):
    n = mesh.shape["dp"]

    to_right = [(i, (i + 1) % n) for i in range(n)]
    to_left = [(i, (i - 1) % n) for i in range(n)]

    def step(x, dy, *arrays):
        near, for_right, for_left = gradients(n, x, dy, *arrays[:3])
        far = (lax.ppermute(for_right, "dp", to_right), lax.ppermute(for_left, "dp", to_left))
        me = lax.axis_index("dp").astype(jnp.int32).reshape(1)
        layers, ff, width = arrays[2].shape
        cut = [a.reshape(layers, ff // CHUNK, CHUNK, width) if i % 3 == 2 else a for i, a in enumerate(arrays)]
        new = adamw(n, me, (near,), cut, 8, True, ())
        new = adamw(n, me, far, cut, 4, False, new)
        return tuple(a.reshape(layers, ff, width) if i % 3 == 2 else a for i, a in enumerate(new))

    return jax.shard_map(
        step,
        mesh=mesh,
        in_specs=(P(("rep", "dp"), None, None),) * 2 + (P(None, None, None),) * 9,
        out_specs=(P("rep", None, None),) * 9,
        check_vma=False,
    )
```

```python
import functools

import jax
import jax.numpy as jnp
from jax import lax
from jax.experimental import pallas as pl
from jax.experimental.pallas import tpu as pltpu
from jax.sharding import PartitionSpec as P

F32 = jnp.float32
BF16 = jnp.bfloat16
CHUNK = 256
TILE = 1024
GSLOTS = 4
FORWARD_PIECES = 4
FORWARD_TILE = 512


def dot(a, b):
    return jnp.dot(a, b, preferred_element_type=F32)


def dot_t(a, b):
    return lax.dot_general(a, b, (((1,), (1,)), ((), ())), preferred_element_type=F32)


def sigmoid(z):
    return 0.5 * jnp.tanh(0.5 * z) + 0.5


def norm_scale(wide):
    return lax.rsqrt(jnp.mean(wide * wide, -1, keepdims=True) + 1e-6)


def step_kernel(
    n, comm,
    x_hbm, dy_hbm, wg_hbm, wu_hbm, wd_hbm, near_hbm, to_right_hbm, to_left_hbm,
    a_all, a_t, d_all, d_t, da, h_all, hid_all, dgu_all, w0_gu, w0_d, s_gu, s_d, part, r1, r2, grad,
    in_sem, w0_sem, w_sem, out_sem, send_sem, recv_sem,
):
    tokens, width = h_all.shape
    layers, _, ff = wg_hbm.shape
    chunks = ff // CHUNK
    tiles = tokens // TILE
    total = layers * chunks
    rows = width // n
    half = rows // 2
    top = layers - 1
    me = lax.axis_index("dp")
    right, left = lax.rem(me + 1, n), lax.rem(me + n - 1, n)
    across = lax.rem(me + 2, n)

    def load(src, dst, sem):
        return pltpu.make_async_copy(src, dst, sem)

    piece_ff = ff // FORWARD_PIECES

    def w0_loads(c):
        cols = pl.ds(c * piece_ff, piece_ff)
        return [
            load(wg_hbm.at[0, :, cols], w0_gu.at[0, :, cols], w0_sem.at[c, 0]),
            load(wu_hbm.at[0, :, cols], w0_gu.at[1, :, cols], w0_sem.at[c, 1]),
            load(wd_hbm.at[0, cols], w0_d.at[cols], w0_sem.at[c, 2]),
        ]

    def x_load(t):
        r = pl.ds(pl.multiple_of(t * FORWARD_TILE, FORWARD_TILE), FORWARD_TILE)
        return load(x_hbm.at[0, r], h_all.at[r], in_sem.at[t, 0])

    def dy_load(t):
        r = pl.ds(pl.multiple_of(t * FORWARD_TILE, FORWARD_TILE), FORWARD_TILE)
        return load(dy_hbm.at[0, r], d_all.at[r], in_sem.at[t, 1])

    def w_loads(s):
        layer = top - s // chunks
        c = pl.ds(pl.multiple_of(lax.rem(s, chunks) * CHUNK, CHUNK), CHUNK)
        slot = lax.rem(s, 2)
        return [
            load(wg_hbm.at[layer, :, c], s_gu.at[slot, :, pl.ds(0, CHUNK)], w_sem.at[slot, 0]),
            load(wu_hbm.at[layer, :, c], s_gu.at[slot, :, pl.ds(CHUNK, CHUNK)], w_sem.at[slot, 1]),
            load(wd_hbm.at[layer, c], s_d.at[slot], w_sem.at[slot, 2]),
        ]

    x_load(0).start()
    for c in range(FORWARD_PIECES):
        for copy in w0_loads(c):
            copy.start()
    barrier = pltpu.get_barrier_semaphore() if comm else None
    if comm:
        for other in (left, right):
            pl.semaphore_signal(barrier, inc=1, device_id={"dp": other}, device_id_type=pl.DeviceIdType.MESH)
    x_load(0).wait()

    def token_rows(t):
        return pl.ds(pl.multiple_of(t * FORWARD_TILE, FORWARD_TILE), FORWARD_TILE)

    def before(t):
        r = token_rows(t)
        x = h_all[r].astype(F32)
        a_all[0, r] = (x * norm_scale(x)).astype(BF16)

    def after(t):
        r = token_rows(t)
        h = (h_all[r].astype(F32) + da[r].astype(BF16).astype(F32)).astype(BF16)
        h_all[r] = h
        wide = h.astype(F32)
        a = (wide * norm_scale(wide)).astype(BF16)
        a_all[1, r] = a
        a_t[:, r] = a.T
        d_t[:, r] = d_all[r].T

    def forward(t, opening):
        a = a_all[0, token_rows(t)]
        acc = None
        for c in range(FORWARD_PIECES):
            cols = pl.ds(c * piece_ff, piece_ff)
            if opening:
                for copy in w0_loads(c):
                    copy.wait()
                if c == 0:
                    for other in range(tokens // FORWARD_TILE):
                        if other:
                            x_load(other).start()
                        dy_load(other).start()
                    for copy in w_loads(0):
                        copy.start()
            gate = dot(a, w0_gu[0, :, cols])
            up = dot(a, w0_gu[1, :, cols])
            if c == 0 and not opening:
                after(t - 1)
            if c == 1 and not opening:
                before(jnp.minimum(t + 1, tokens // FORWARD_TILE - 1))
            hid = (gate * sigmoid(gate) * up).astype(BF16)
            term = dot(hid, w0_d[cols])
            acc = term if acc is None else acc + term
        da[token_rows(t)] = acc

    before(0)
    forward(0, True)
    for t in range(tokens // FORWARD_TILE):
        if t:
            x_load(t).wait()
        dy_load(t).wait()
    before(1)

    def forward_rest(t, carry):
        forward(t, False)
        return carry

    lax.fori_loop(1, tokens // FORWARD_TILE, forward_rest, 0)
    after(tokens // FORWARD_TILE - 1)

    def piece(j, which):
        if which is None:
            return pl.ds(pl.multiple_of(j * rows, rows), rows)
        return pl.ds(pl.multiple_of(j * rows + which * half, half), half)

    def copies(kind, q):
        par = lax.rem(q, 2)
        g = lax.rem(q, GSLOTS)
        if kind == 0:
            pairs = [(part.at[par, :, piece(across, d)], r1.at[par, d]) for d in range(2)]
        elif kind == 1:
            pairs = [(part.at[par, :, piece(to, None)], r2.at[par, d]) for d, to in enumerate((right, left))]
        else:
            pairs = [(grad.at[g, 0], grad.at[g, 1 + d]) for d in range(2)]
        return [
            pltpu.make_async_remote_copy(
                src_ref=src, dst_ref=dst, send_sem=send_sem.at[kind, d, par], recv_sem=recv_sem.at[kind, d, par],
                device_id={"dp": to}, device_id_type=pl.DeviceIdType.MESH,
            )
            for d, ((src, dst), to) in enumerate(zip(pairs, (right, left)))
        ]

    def landed(kind, q):
        for copy in copies(kind, q):
            copy.wait_recv()
            copy.wait_send()

    def send(kind, q):
        for copy in copies(kind, q):
            copy.start()

    def pass_on(q):
        landed(0, q)
        par = lax.rem(q, 2)
        for d, to in enumerate((right, left)):
            at = piece(to, d)
            part[par, :, at] = (part[par, :, at].astype(F32) + r1[par, d].astype(F32)).astype(BF16)
        send(1, q)

    def finish(q):
        landed(1, q)
        par = lax.rem(q, 2)
        mine = part[par, :, piece(me, None)].astype(F32)
        grad[lax.rem(q, GSLOTS), 0] = (mine + r2[par, 0].astype(F32) + r2[par, 1].astype(F32)).astype(BF16)
        send(2, q)

    def out_copies(q):
        g, par = lax.rem(q, GSLOTS), lax.rem(q, 2)
        return [
            pltpu.make_async_copy(grad.at[g], near_hbm.at[q], out_sem.at[par, 0]),
            pltpu.make_async_copy(grad.at[g, 1, :, pl.ds(0, half)], to_right_hbm.at[q], out_sem.at[par, 1]),
            pltpu.make_async_copy(grad.at[g, 2, :, pl.ds(half, half)], to_left_hbm.at[q], out_sem.at[par, 2]),
        ]

    def collect(q):
        landed(2, q)
        for copy in out_copies(q):
            copy.start()

    def settle(q):
        for copy in out_copies(q):
            copy.wait()

    def tile_body(layer, slot, t, with_da, fresh):
        r = pl.ds(pl.multiple_of(t * TILE, TILE), TILE)
        gu = dot(a_all[layer, r], s_gu[slot])
        gate, up = gu[:, :CHUNK], gu[:, CHUNK:]
        dhid = dot_t(d_all[r], s_d[slot]).astype(BF16).astype(F32)
        sig = sigmoid(gate)
        silu = gate * sig
        hid_all[r] = (silu * up).astype(BF16)
        dgate = (dhid * up * (sig + silu * (1.0 - sig))).astype(BF16)
        dup = (dhid * silu).astype(BF16)
        dgu_all[r, :CHUNK] = dgate
        dgu_all[r, CHUNK:] = dup
        if with_da:
            term = dot_t(jnp.concatenate([dgate, dup], axis=1), s_gu[slot])
            da[r] = jnp.where(fresh, 0.0, da[r]) + term

    def service(guard, fn, q):
        if not comm:
            return
        if guard is None:
            fn(q)
        else:
            pl.when(guard)(lambda: fn(q))

    def chunk_step(s, with_da):
        layer = top - s // chunks
        slot = lax.rem(s, 2)
        for copy in w_loads(s):
            copy.wait()

        @pl.when(s + 1 < total)
        def _():
            for copy in w_loads(s + 1):
                copy.start()

        fresh = lax.rem(s, chunks) == 0
        body = lambda t, c: (tile_body(layer, slot, t, with_da, fresh), c)[1]
        ahead = tiles - 1
        lax.fori_loop(0, ahead, body, 0)
        service(s >= 3, finish, s - 2)
        service(s >= 4, settle, s - 4)
        service(s >= 3, collect, s - 3)
        service(s >= 1, pass_on, s - 1)
        lax.fori_loop(ahead, tiles, body, 0)
        dw = dot(a_t[...], dgu_all[...])
        part[slot, 0] = dw[:, :CHUNK].astype(BF16)
        part[slot, 1] = dw[:, CHUNK:].astype(BF16)
        dd = dot(d_t[...], hid_all[...])
        for k in range(width // CHUNK):
            b = pl.ds(k * CHUNK, CHUNK)
            part[slot, 2, b] = dd[k * CHUNK : (k + 1) * CHUNK].T.astype(BF16)
        if comm:
            send(0, s)
        service(s == 1, finish, s - 1)

    def turn(t, carry):
        r = pl.ds(pl.multiple_of(t * TILE, TILE), TILE)
        by_a = da[r].astype(BF16).astype(F32)
        h = h_all[r].astype(F32)
        scale = norm_scale(h)
        inner = jnp.mean(by_a * h, -1, keepdims=True)
        by_h = d_all[r].astype(F32) + (by_a * scale - h * (scale * scale * scale * inner))
        by_h = by_h.astype(BF16)
        d_all[r] = by_h
        d_t[:, r] = by_h.T
        a_t[:, r] = a_all[0, r].T
        return carry

    if comm:
        pl.semaphore_wait(barrier, 2)

    def upper(s, carry):
        chunk_step(s, True)
        return carry

    def lower(s, carry):
        chunk_step(s, False)
        return carry

    lax.fori_loop(0, chunks, upper, 0)
    lax.fori_loop(0, tiles, turn, 0)
    lax.fori_loop(chunks, total, lower, 0)

    if comm:
        last = total - 1
        finish(last - 1)
        settle(last - 3)
        collect(last - 2)
        pass_on(last)
        finish(last)
        settle(last - 2)
        collect(last - 1)
        collect(last)
        settle(last - 1)
        settle(last)


def gradients(n, x, dy, wg, wu, wd, comm=True):
    _, tokens, width = x.shape
    layers, _, ff = wg.shape
    assert layers == 2 and n == 4
    total = layers * ff // CHUNK
    rows = width // n
    anywhere = pl.BlockSpec(memory_space=pl.ANY)
    return pl.pallas_call(
        functools.partial(step_kernel, n, comm),
        out_shape=[
            jax.ShapeDtypeStruct((total, 3, 3, rows, CHUNK), BF16),
            jax.ShapeDtypeStruct((total, 3, rows // 2, CHUNK), BF16),
            jax.ShapeDtypeStruct((total, 3, rows // 2, CHUNK), BF16),
        ],
        in_specs=[anywhere] * 5,
        out_specs=[anywhere] * 3,
        scratch_shapes=[
            pltpu.VMEM((2, tokens, width), BF16),
            pltpu.VMEM((width, tokens), BF16),
            pltpu.VMEM((tokens, width), BF16),
            pltpu.VMEM((width, tokens), BF16),
            pltpu.VMEM((tokens, width), F32),
            pltpu.VMEM((tokens, width), BF16),
            pltpu.VMEM((tokens, CHUNK), BF16),
            pltpu.VMEM((tokens, 2 * CHUNK), BF16),
            pltpu.VMEM((2, width, ff), BF16),
            pltpu.VMEM((ff, width), BF16),
            pltpu.VMEM((2, width, 2 * CHUNK), BF16),
            pltpu.VMEM((2, CHUNK, width), BF16),
            pltpu.VMEM((2, 3, width, CHUNK), BF16),
            pltpu.VMEM((2, 2, 3, rows // 2, CHUNK), BF16),
            pltpu.VMEM((2, 2, 3, rows, CHUNK), BF16),
            pltpu.VMEM((GSLOTS, 3, 3, rows, CHUNK), BF16),
            pltpu.SemaphoreType.DMA((tokens // FORWARD_TILE, 2)),
            pltpu.SemaphoreType.DMA((FORWARD_PIECES, 3)),
            pltpu.SemaphoreType.DMA((2, 3)),
            pltpu.SemaphoreType.DMA((2, 3)),
            pltpu.SemaphoreType.DMA((3, 2, 2)),
            pltpu.SemaphoreType.DMA((3, 2, 2)),
        ],
        compiler_params=pltpu.CompilerParams(
            collective_id=0 if comm else None, has_side_effects=True, vmem_limit_bytes=67043328
        ),
        name="gradients",
    )(x, dy, wg, wu, wd)


def adamw_math(w, m, v, g):
    m = 0.9 * m + 0.1 * g
    v = 0.95 * v + 0.05 * g * g
    step = m * lax.rsqrt(v + 1e-8) + 0.1 * w
    return (w - 0.02 * step).astype(BF16), m, v


def adamw_kernel(gs, me_ref, *refs):
    parts, ins, outs = refs[:gs], refs[gs : gs + 9], refs[-9:]
    group = parts[0].shape[0]
    for j in range(group):
        cols = pl.ds(j * CHUNK, CHUNK)
        for i in range(3):
            g = parts[0][j, 0, i] if gs == 1 else jnp.concatenate([p[j, i] for p in parts], axis=0)
            at = (0, slice(None), cols) if i < 2 else (0, j)
            new = adamw_math(ins[i][at].astype(F32), ins[3 + i][at], ins[6 + i][at], g.astype(F32))
            for k in range(3):
                outs[3 * k + i][at] = new[k]


def adamw(n, me, gs, arrays, group, near, before):
    layers, width, ff = arrays[0].shape
    groups = ff // CHUNK // group
    rows = width // n
    per = CHUNK // rows

    def row(rel, me):
        ahead = jnp.where(rel == 0, 0, jnp.where(rel == 1, n - 1, 1)) if near else n // 2
        return lax.rem(me[0] + ahead, n)

    def wide_map(s, rel, c, me):
        return layers - 1 - s, row(rel, me), c

    def tall_map(s, rel, c, me):
        at = row(rel, me)
        return layers - 1 - s, c, lax.rem(at, per), at // per

    wide = pl.BlockSpec((1, rows, group * CHUNK), wide_map, pipeline_mode=pl.Buffered(2))
    tall = pl.BlockSpec((1, group, rows, CHUNK), tall_map, pipeline_mode=pl.Buffered(2))
    specs = [wide, wide, tall] * 3
    outs = [pl.BlockSpec(b.block_shape, b.index_map) for b in specs]
    if near:
        g_specs = [pl.BlockSpec((group, 1, 3, rows, CHUNK), lambda s, rel, c, me: (s * groups + c, rel, 0, 0, 0))]
    else:
        g_specs = [pl.BlockSpec((group, 3, rows // 2, CHUNK), lambda s, rel, c, me: (s * groups + c, 0, 0, 0))] * 2
    shares = 3 if near else 1
    size = layers * ff * 3 * rows * shares
    return pl.pallas_call(
        functools.partial(adamw_kernel, len(gs)),
        grid_spec=pltpu.PrefetchScalarGridSpec(
            num_scalar_prefetch=1,
            grid=(layers, shares, groups),
            in_specs=g_specs + specs + [pl.BlockSpec(memory_space=pl.ANY)] * len(before),
            out_specs=outs,
        ),
        out_shape=[jax.ShapeDtypeStruct(a.shape, a.dtype) for a in arrays],
        input_output_aliases={1 + len(gs) + 9 + i: i for i in range(len(before))},
        compiler_params=pltpu.CompilerParams(vmem_limit_bytes=67043328),
        cost_estimate=pl.CostEstimate(flops=size * 2000, bytes_accessed=size * 22, transcendentals=size),
        name="adamw_near" if near else "adamw_across",
    )(me, *gs, *arrays, *before)


def solution(mesh):
    n = mesh.shape["dp"]

    to_right = [(i, (i + 1) % n) for i in range(n)]
    to_left = [(i, (i - 1) % n) for i in range(n)]

    def step(x, dy, *arrays):
        near, for_right, for_left = gradients(n, x, dy, *arrays[:3])
        far = (lax.ppermute(for_right, "dp", to_right), lax.ppermute(for_left, "dp", to_left))
        me = lax.axis_index("dp").astype(jnp.int32).reshape(1)
        layers, ff, width = arrays[2].shape
        cut = [a.reshape(layers, ff // CHUNK, CHUNK, width) if i % 3 == 2 else a for i, a in enumerate(arrays)]
        new = adamw(n, me, (near,), cut, 8, True, ())
        new = adamw(n, me, far, cut, 8, False, new)
        return tuple(a.reshape(layers, ff, width) if i % 3 == 2 else a for i, a in enumerate(new))

    return jax.shard_map(
        step,
        mesh=mesh,
        in_specs=(P(("rep", "dp"), None, None),) * 2 + (P(None, None, None),) * 9,
        out_specs=(P("rep", None, None),) * 9,
        check_vma=False,
    )
```
